32 devices in a mesh: win: 16 (over z, y, core), head: 2 (over x).
Axes of the slice: x: 2, y: 2, z: 4, core: 2. Of those that a mesh axis runs over, the one named last changes fastest.
Arguments:
- qkv: bfloat16 [3, 16, 96, 48, 1024], P(None, 'win', 'head'), may hold values from -10 to 10
Outputs:
- attended: bfloat16 [16, 96, 48, 1024], P('win', 'head')
The draws below stay inside these ranges and needn't reach their ends.
All inputs are finite; a program needn't handle non-finite values.
Results may differ from the reference program's by a relative error of at most 0.0047.
Values may be sent and summed in bfloat16 or wider, within the bound.
A program may use at most 192 MiB of HBM per device.

```python
import math
import jax
import jax.numpy as jnp
from jax import lax

HEADS = 8
HEAD_DIM = 128
WIN = 48
LAT_WIN = 4
ROWS = 192
HALF_ROWS = 96
LON_BANDS = 8


def draw_qkv(key, part):
    channels = HEADS * HEAD_DIM
    blocks = 2 * LON_BANDS
    full_shape = (3, blocks, HALF_ROWS, WIN, channels)
    key_base = jax.random.fold_in(jax.random.fold_in(key, 7), 0)
    values = jnp.clip(jax.random.normal(key_base, full_shape, jnp.float32), -6.0, 6.0)
    return values.astype(jnp.bfloat16)


def setup_inputs(seed: int = 0) -> dict:
    seeds = jax.random.split(jax.random.key(seed), 2)
    qkv = draw_qkv(jax.random.fold_in(seeds[1], 71), 0)
    return {"qkv": qkv}


def attend(queries, keys, values, labels_query, labels_key):
    score_scale = 1.0 / math.sqrt(queries.shape[-1])
    scores = jnp.einsum('qhd,khd->hqk', queries.astype(jnp.float32), keys.astype(jnp.float32)) * score_scale
    allowed = labels_query[:, None] == labels_key[None, :]
    scores = jnp.where(allowed[None], scores, -jnp.inf)
    row_max = lax.optimization_barrier(jnp.max(scores, axis=-1, keepdims=True))
    weights = jnp.exp(scores - row_max)
    row_total = lax.optimization_barrier(jnp.sum(weights, axis=-1, keepdims=True))
    rounded = lax.optimization_barrier(weights.astype(jnp.bfloat16)).astype(jnp.float32)
    mixture = jnp.einsum('hqk,khd->qhd', rounded, values.astype(jnp.float32))
    return (mixture / jnp.transpose(row_total, (1, 0, 2))).astype(jnp.bfloat16)

def reference(qkv):
    half_cols = WIN // 2
    channels = HEADS * HEAD_DIM
    bands = qkv.reshape(3, LON_BANDS, ROWS, WIN, channels)
    rolled_rows = jnp.roll(jnp.arange(ROWS, dtype=jnp.int32), -half_cols)
    row_labels = (rolled_rows < half_cols).astype(jnp.int32)
    label_parts = jnp.broadcast_to(row_labels.reshape(LAT_WIN, WIN, 1), (LAT_WIN, WIN, WIN)).reshape(LAT_WIN, WIN * WIN)

    def one_window(lon_index):
        east_index = ((lon_index + 1) % LON_BANDS).astype(jnp.int32)
        own_band = lax.dynamic_index_in_dim(bands, lon_index, 1, keepdims=False)
        east_band = lax.dynamic_index_in_dim(bands, east_index, 1, keepdims=False)
        window = jnp.concatenate([own_band[:, :, half_cols:], east_band[:, :, :half_cols]], axis=2)
        window = jnp.roll(window, -half_cols, axis=1)
        window_parts = window.reshape(3, LAT_WIN, WIN * WIN, HEADS, HEAD_DIM)

        def one_band(pieces):
            window_part, label_part = pieces
            return attend(window_part[0], window_part[1], window_part[2], label_part, label_part)
        result = lax.map(one_band, (jnp.moveaxis(window_parts, 1, 0), label_parts))
        result = result.reshape(ROWS, WIN, channels)
        return jnp.roll(result, half_cols, axis=0)
    outputs = lax.map(one_window, jnp.arange(LON_BANDS, dtype=jnp.int32))
    joined = jnp.concatenate([jnp.roll(outputs[:, :, half_cols:], 1, axis=0), outputs[:, :, :half_cols]], axis=2)
    return joined.reshape(2 * LON_BANDS, HALF_ROWS, WIN, channels)
```

```python
import functools
import math

import jax
import jax.numpy as jnp
from jax import lax
from jax.experimental import pallas as pl
from jax.experimental.pallas import tpu as pltpu
from jax.sharding import PartitionSpec as P

HEAD_DIM = 128


def from_behind(shard, axis, by):
    count = lax.axis_size(axis)
    return lax.ppermute(shard, axis, [(i, (i + by) % count) for i in range(count)])


def partner(value, axis, apart):
    mask = 2**apart
    pairs = [(source, source ^ mask) for source in range(lax.axis_size(axis))]
    return lax.ppermute(value, axis, pairs)


def attend(queries, keys, values, labels_query, labels_key):
    query_count, head_count, head_width = queries.shape
    block_rows = math.gcd(query_count, 576)
    score_scale = 1.0 / math.sqrt(head_width)

    def one_block(pieces):
        query_block, label_block = pieces
        scores = (
            jnp.einsum("qhd,khd->hqk", query_block, keys, preferred_element_type=jnp.float32)
            * score_scale
        )
        allowed = label_block[:, None] == labels_key[None, :]
        scores = jnp.where(allowed[None], scores, -jnp.inf)
        row_max = jnp.max(scores, axis=-1, keepdims=True)
        weights = jnp.exp(scores - row_max)
        row_total = jnp.sum(weights, axis=-1, keepdims=True)
        mixture = jnp.einsum(
            "hqk,khd->qhd", weights.astype(jnp.bfloat16), values, preferred_element_type=jnp.float32
        )
        return (mixture / jnp.transpose(row_total, (1, 0, 2))).astype(jnp.bfloat16)

    query_blocks = queries.reshape(query_count // block_rows, block_rows, head_count, head_width)
    label_blocks = labels_query.reshape(query_count // block_rows, block_rows)
    return lax.map(one_block, (query_blocks, label_blocks)).reshape(
        query_count, head_count, head_width
    )


def window_attention(window, labels):
    row_count, side_cells, channels = (window.shape[1], window.shape[2], window.shape[3])
    head_count = channels // HEAD_DIM
    window_parts = window.reshape(
        3, row_count // side_cells, side_cells * side_cells, head_count, HEAD_DIM
    )
    label_parts = labels.reshape(row_count // side_cells, side_cells * side_cells)
    outputs = []
    for window_row in range(row_count // side_cells):
        outputs.append(
            attend(
                window_parts[0, window_row],
                window_parts[1, window_row],
                window_parts[2, window_row],
                label_parts[window_row],
                label_parts[window_row],
            )
        )
    return jnp.stack(outputs).reshape(row_count, side_cells, channels)


def general_body(qkv):
    side_cells = qkv.shape[3]
    half_cols = side_cells // 2
    tokens = qkv[:, 0]
    arrived = from_behind(tokens[:, :, :half_cols], "win", -2)
    tokens = jnp.concatenate([tokens[:, :, half_cols:], arrived], axis=2)
    head_view = lax.all_to_all(tokens, "head", split_axis=3, concat_axis=1, tiled=True)
    half_rows = head_view.shape[1]
    crossing = partner(head_view[:, :half_cols], "win", 0)
    extended = jnp.concatenate([head_view[:, half_cols:], crossing], axis=1)
    lat_half = lax.axis_index("win") % 2
    row_index = jnp.arange(half_rows, dtype=jnp.int32)[:, None]
    wrapped = jnp.logical_and(lat_half == 1, row_index >= half_rows - half_cols)
    labels = jnp.broadcast_to(jnp.where(wrapped, 1, 0).astype(jnp.int32), (half_rows, side_cells))
    result = window_attention(extended, labels)
    returned = partner(result[half_rows - half_cols :], "win", 0)
    row_fixed = jnp.concatenate([returned, result[: half_rows - half_cols]], axis=0)
    restored = lax.all_to_all(row_fixed, "head", split_axis=0, concat_axis=2, tiled=True)
    from_west = from_behind(restored[:, half_cols:], "win", 2)
    restored = jnp.concatenate([from_west, restored[:, :half_cols]], axis=1)
    return restored[None]


HEADS_PER_CHUNK = 2


def attend_kernel(block_rows, flag_ref, *refs):
    quarters, outs = refs[:4], refs[4:8]
    q_all, k_all, v_all, o_all, scores_a, scores_b, max_a, max_b = refs[8:]
    part, width = quarters[0].shape[1:]
    tokens = 4 * part
    factor = math.log2(math.e) / math.sqrt(width)
    for index, quarter in enumerate(quarters):
        rows = pl.ds(index * part, part)
        q_all[rows, :] = quarter[0]
        k_all[rows, :] = quarter[1]
        v_all[rows, pl.ds(0, width)] = quarter[2]
    v_all[:, pl.ds(width, width)] = jnp.ones((tokens, width), jnp.bfloat16)

    def run(first, row_count, key_first, key_count):
        keys = pl.ds(key_first, key_count)
        blocks = row_count // block_rows

        def rows_of(block):
            return pl.ds(pl.multiple_of(first + block * block_rows, block_rows), block_rows)

        def score(block, scores, row_max):
            s = lax.dot_general(
                q_all[rows_of(block), :],
                k_all[keys, :],
                (((1,), (1,)), ((), ())),
                preferred_element_type=jnp.float32,
            )
            scores[:, pl.ds(0, key_count)] = s
            row_max[...] = jnp.broadcast_to(
                jnp.max(s, axis=1, keepdims=True) * factor, row_max.shape
            )

        def mix(block, scores, row_max):
            top = row_max[:, pl.ds(0, 1)]
            weights = jnp.exp2(scores[:, pl.ds(0, key_count)] * factor - top)
            mixture = jnp.dot(
                weights.astype(jnp.bfloat16), v_all[keys, :], preferred_element_type=jnp.float32
            )
            o_all[rows_of(block), :] = (mixture[:, :width] / mixture[:, width:]).astype(
                jnp.bfloat16
            )

        score(0, scores_a, max_a)

        def pair(step, carry):
            score(2 * step + 1, scores_b, max_b)
            mix(2 * step, scores_a, max_a)
            score(jnp.minimum(2 * step + 2, blocks - 1), scores_a, max_a)
            mix(2 * step + 1, scores_b, max_b)
            return carry

        lax.fori_loop(0, blocks // 2, pair, 0)

    @pl.when(flag_ref[0] == 0)
    def _():
        run(0, tokens, 0, tokens)

    @pl.when(flag_ref[0] != 0)
    def _():
        run(0, tokens // 2, 0, tokens // 2)
        run(tokens // 2, tokens // 2, tokens // 2, tokens // 2)

    for index, out in enumerate(outs):
        out[...] = o_all[pl.ds(index * part, part), :]


def attend_quarters(flag, quarters):
    part, width = quarters[0].shape[1:]
    heads = width // HEAD_DIM
    tokens = 4 * part
    block_rows = part // 3
    quarter_spec = pl.BlockSpec((3, part, HEAD_DIM), lambda h: (0, 0, h))
    out_spec = pl.BlockSpec((part, HEAD_DIM), lambda h: (0, h))
    return pl.pallas_call(
        functools.partial(attend_kernel, block_rows),
        grid=(heads,),
        in_specs=[pl.BlockSpec(memory_space=pltpu.SMEM)] + [quarter_spec] * 4,
        out_specs=[out_spec] * 4,
        out_shape=[jax.ShapeDtypeStruct((part, width), jnp.bfloat16)] * 4,
        scratch_shapes=[
            pltpu.VMEM((tokens, HEAD_DIM), jnp.bfloat16),
            pltpu.VMEM((tokens, HEAD_DIM), jnp.bfloat16),
            pltpu.VMEM((tokens, 2 * HEAD_DIM), jnp.bfloat16),
            pltpu.VMEM((tokens, HEAD_DIM), jnp.bfloat16),
            pltpu.VMEM((block_rows, tokens), jnp.float32),
            pltpu.VMEM((block_rows, tokens), jnp.float32),
            pltpu.VMEM((block_rows, HEAD_DIM), jnp.float32),
            pltpu.VMEM((block_rows, HEAD_DIM), jnp.float32),
        ],
        compiler_params=pltpu.CompilerParams(
            dimension_semantics=("arbitrary",), vmem_limit_bytes=40 * 2**20
        ),
        cost_estimate=pl.CostEstimate(
            flops=8 * heads * tokens * tokens * HEAD_DIM,
            transcendentals=heads * tokens * tokens,
            bytes_accessed=4 * tokens * width * 2,
        ),
    )(flag, *quarters)


def window_body(row_blocks, bands, qkv):
    tokens = qkv[:, 0]
    side, channels = tokens.shape[2], tokens.shape[3]
    half = side // 2
    axes = ("win", "head")

    def shift(value, rows, columns):
        pairs = []
        for band in range(bands):
            for row in range(row_blocks):
                target = ((band + columns) % bands) * row_blocks + (row + rows) % row_blocks
                pairs.append((band * row_blocks + row, target))
        return lax.ppermute(value, axes, pairs)

    row_block = lax.axis_index(axes) % row_blocks
    flag = (row_block == row_blocks - 1).astype(jnp.int32).reshape(1)
    low, high = slice(0, half), slice(half, side)
    chunk_width = HEADS_PER_CHUNK * HEAD_DIM
    received = []
    for start in range(0, channels, chunk_width):
        lanes = slice(start, start + chunk_width)

        def piece(rows, columns):
            return tokens[:, rows, columns, lanes].reshape(3, half * half, chunk_width)

        received.append(
            (
                piece(high, high),
                shift(piece(high, low), 0, -1),
                shift(piece(low, high), -1, 0),
                shift(piece(low, low), -1, -1),
            )
        )
    results = []
    for quarters in received:
        own, east, south, corner = attend_quarters(flag, quarters)
        results.append((own, shift(east, 0, 1), shift(south, 1, 0), shift(corner, 1, 1)))
    own, east, south, corner = (
        jnp.concatenate(
            [result[index].reshape(half, half, chunk_width) for result in results], axis=2
        )
        for index in range(4)
    )
    top = jnp.concatenate([corner, south], axis=1)
    bottom = jnp.concatenate([east, own], axis=1)
    return jnp.concatenate([top, bottom], axis=0)[None]


def solution(mesh):
    in_specs = (P(None, "win", "head", None, None),)
    out_specs = P("win", "head", None, None)
    win_count, head_count = mesh.shape["win"], mesh.shape["head"]

    def body(qkv):
        if qkv.shape[2] == qkv.shape[3]:
            return window_body(2 * head_count, win_count // 2, qkv)
        return general_body(qkv)

    return jax.shard_map(body, mesh=mesh, in_specs=in_specs, out_specs=out_specs, check_vma=False)
```

```python
import functools
import math

import jax
import jax.numpy as jnp
from jax import lax
from jax.experimental import pallas as pl
from jax.experimental.pallas import tpu as pltpu
from jax.sharding import PartitionSpec as P

HEAD_DIM = 128


def from_behind(shard, axis, by):
    count = lax.axis_size(axis)
    return lax.ppermute(shard, axis, [(i, (i + by) % count) for i in range(count)])


def partner(value, axis, apart):
    mask = 2**apart
    pairs = [(source, source ^ mask) for source in range(lax.axis_size(axis))]
    return lax.ppermute(value, axis, pairs)


def attend(queries, keys, values, labels_query, labels_key):
    query_count, head_count, head_width = queries.shape
    block_rows = math.gcd(query_count, 576)
    score_scale = 1.0 / math.sqrt(head_width)

    def one_block(pieces):
        query_block, label_block = pieces
        scores = (
            jnp.einsum("qhd,khd->hqk", query_block, keys, preferred_element_type=jnp.float32)
            * score_scale
        )
        allowed = label_block[:, None] == labels_key[None, :]
        scores = jnp.where(allowed[None], scores, -jnp.inf)
        row_max = jnp.max(scores, axis=-1, keepdims=True)
        weights = jnp.exp(scores - row_max)
        row_total = jnp.sum(weights, axis=-1, keepdims=True)
        mixture = jnp.einsum(
            "hqk,khd->qhd", weights.astype(jnp.bfloat16), values, preferred_element_type=jnp.float32
        )
        return (mixture / jnp.transpose(row_total, (1, 0, 2))).astype(jnp.bfloat16)

    query_blocks = queries.reshape(query_count // block_rows, block_rows, head_count, head_width)
    label_blocks = labels_query.reshape(query_count // block_rows, block_rows)
    return lax.map(one_block, (query_blocks, label_blocks)).reshape(
        query_count, head_count, head_width
    )


def window_attention(window, labels):
    row_count, side_cells, channels = (window.shape[1], window.shape[2], window.shape[3])
    head_count = channels // HEAD_DIM
    window_parts = window.reshape(
        3, row_count // side_cells, side_cells * side_cells, head_count, HEAD_DIM
    )
    label_parts = labels.reshape(row_count // side_cells, side_cells * side_cells)
    outputs = []
    for window_row in range(row_count // side_cells):
        outputs.append(
            attend(
                window_parts[0, window_row],
                window_parts[1, window_row],
                window_parts[2, window_row],
                label_parts[window_row],
                label_parts[window_row],
            )
        )
    return jnp.stack(outputs).reshape(row_count, side_cells, channels)


def general_body(qkv):
    side_cells = qkv.shape[3]
    half_cols = side_cells // 2
    tokens = qkv[:, 0]
    arrived = from_behind(tokens[:, :, :half_cols], "win", -2)
    tokens = jnp.concatenate([tokens[:, :, half_cols:], arrived], axis=2)
    head_view = lax.all_to_all(tokens, "head", split_axis=3, concat_axis=1, tiled=True)
    half_rows = head_view.shape[1]
    crossing = partner(head_view[:, :half_cols], "win", 0)
    extended = jnp.concatenate([head_view[:, half_cols:], crossing], axis=1)
    lat_half = lax.axis_index("win") % 2
    row_index = jnp.arange(half_rows, dtype=jnp.int32)[:, None]
    wrapped = jnp.logical_and(lat_half == 1, row_index >= half_rows - half_cols)
    labels = jnp.broadcast_to(jnp.where(wrapped, 1, 0).astype(jnp.int32), (half_rows, side_cells))
    result = window_attention(extended, labels)
    returned = partner(result[half_rows - half_cols :], "win", 0)
    row_fixed = jnp.concatenate([returned, result[: half_rows - half_cols]], axis=0)
    restored = lax.all_to_all(row_fixed, "head", split_axis=0, concat_axis=2, tiled=True)
    from_west = from_behind(restored[:, half_cols:], "win", 2)
    restored = jnp.concatenate([from_west, restored[:, :half_cols]], axis=1)
    return restored[None]


CHUNKS = 4


def attend_kernel(block_rows, flag_ref, *refs):
    quarters, outs = refs[:4], refs[4:8]
    q_all, k_all, v_all, o_all, scores_a, scores_b, max_a, max_b = refs[8:]
    part, width = quarters[0].shape[1:]
    tokens = 4 * part
    factor = math.log2(math.e) / math.sqrt(width)
    for index, quarter in enumerate(quarters):
        rows = pl.ds(index * part, part)
        q_all[rows, :] = quarter[0]
        k_all[rows, :] = quarter[1]
        v_all[rows, pl.ds(0, width)] = quarter[2]
    v_all[:, pl.ds(width, width)] = jnp.ones((tokens, width), jnp.bfloat16)

    def run(first, row_count, key_first, key_count):
        keys = pl.ds(key_first, key_count)
        blocks = row_count // block_rows

        def rows_of(block):
            return pl.ds(pl.multiple_of(first + block * block_rows, block_rows), block_rows)

        def score(block, scores, row_max):
            s = lax.dot_general(
                q_all[rows_of(block), :],
                k_all[keys, :],
                (((1,), (1,)), ((), ())),
                preferred_element_type=jnp.float32,
            )
            scores[:, pl.ds(0, key_count)] = s
            row_max[...] = jnp.broadcast_to(
                jnp.max(s, axis=1, keepdims=True) * factor, row_max.shape
            )

        def mix(block, scores, row_max):
            top = row_max[:, pl.ds(0, 1)]
            weights = jnp.exp2(scores[:, pl.ds(0, key_count)] * factor - top)
            mixture = jnp.dot(
                weights.astype(jnp.bfloat16), v_all[keys, :], preferred_element_type=jnp.float32
            )
            o_all[rows_of(block), :] = (mixture[:, :width] / mixture[:, width:]).astype(
                jnp.bfloat16
            )

        score(0, scores_a, max_a)

        def pair(step, carry):
            score(2 * step + 1, scores_b, max_b)
            mix(2 * step, scores_a, max_a)
            score(jnp.minimum(2 * step + 2, blocks - 1), scores_a, max_a)
            mix(2 * step + 1, scores_b, max_b)
            return carry

        lax.fori_loop(0, blocks // 2, pair, 0)

    @pl.when(flag_ref[0] == 0)
    def _():
        run(0, tokens, 0, tokens)

    @pl.when(flag_ref[0] != 0)
    def _():
        run(0, tokens // 2, 0, tokens // 2)
        run(tokens // 2, tokens // 2, tokens // 2, tokens // 2)

    for index, out in enumerate(outs):
        out[...] = o_all[pl.ds(index * part, part), :]


def attend_quarters(flag, quarters):
    part, width = quarters[0].shape[1:]
    heads = width // HEAD_DIM
    tokens = 4 * part
    block_rows = part // 3
    quarter_spec = pl.BlockSpec((3, part, HEAD_DIM), lambda h: (0, 0, h))
    out_spec = pl.BlockSpec((part, HEAD_DIM), lambda h: (0, h))
    return pl.pallas_call(
        functools.partial(attend_kernel, block_rows),
        grid=(heads,),
        in_specs=[pl.BlockSpec(memory_space=pltpu.SMEM)] + [quarter_spec] * 4,
        out_specs=[out_spec] * 4,
        out_shape=[jax.ShapeDtypeStruct((part, width), jnp.bfloat16)] * 4,
        scratch_shapes=[
            pltpu.VMEM((tokens, HEAD_DIM), jnp.bfloat16),
            pltpu.VMEM((tokens, HEAD_DIM), jnp.bfloat16),
            pltpu.VMEM((tokens, 2 * HEAD_DIM), jnp.bfloat16),
            pltpu.VMEM((tokens, HEAD_DIM), jnp.bfloat16),
            pltpu.VMEM((block_rows, tokens), jnp.float32),
            pltpu.VMEM((block_rows, tokens), jnp.float32),
            pltpu.VMEM((block_rows, HEAD_DIM), jnp.float32),
            pltpu.VMEM((block_rows, HEAD_DIM), jnp.float32),
        ],
        compiler_params=pltpu.CompilerParams(
            dimension_semantics=("arbitrary",), vmem_limit_bytes=40 * 2**20
        ),
        cost_estimate=pl.CostEstimate(
            flops=8 * heads * tokens * tokens * HEAD_DIM,
            transcendentals=heads * tokens * tokens,
            bytes_accessed=4 * tokens * width * 2,
        ),
    )(flag, *quarters)


def assemble_kernel(widths, *refs):
    pieces, out = refs[:-1], refs[-1]
    half = out.shape[2] // 2
    start = 0
    for index, width in enumerate(widths):
        own, east, south, corner = pieces[4 * index : 4 * index + 4]
        lanes = pl.ds(start, width)
        out[0, :, pl.ds(0, half), lanes] = corner[...]
        out[0, :, pl.ds(half, half), lanes] = south[...]
        out[1, :, pl.ds(0, half), lanes] = east[...]
        out[1, :, pl.ds(half, half), lanes] = own[...]
        start += width


def assemble(half, results):
    widths = [result[0].shape[1] for result in results]
    channels = sum(widths)
    rows = max(math.gcd(half, 3), 1)
    pieces = [piece.reshape(half, half, piece.shape[1]) for result in results for piece in result]
    return pl.pallas_call(
        functools.partial(assemble_kernel, widths),
        grid=(half // rows,),
        in_specs=[
            pl.BlockSpec((rows, half, piece.shape[2]), lambda r: (r, 0, 0)) for piece in pieces
        ],
        out_specs=pl.BlockSpec((2, rows, 2 * half, channels), lambda r: (0, r, 0, 0)),
        out_shape=jax.ShapeDtypeStruct((2, half, 2 * half, channels), jnp.bfloat16),
        compiler_params=pltpu.CompilerParams(
            dimension_semantics=("arbitrary",), vmem_limit_bytes=40 * 2**20
        ),
    )(*pieces)


def head_chunks(heads):
    size = max(heads // CHUNKS, 1)
    sizes = [size] * (heads // size)
    if size > 1:
        sizes[-1:] = [size - size // 2, size // 2]
    return sizes + [1] * (heads - sum(sizes))


def window_body(row_blocks, bands, qkv):
    tokens = qkv[:, 0]
    side, channels = tokens.shape[2], tokens.shape[3]
    half = side // 2
    axes = ("win", "head")

    def shift(value, rows, columns):
        pairs = []
        for band in range(bands):
            for row in range(row_blocks):
                target = ((band + columns) % bands) * row_blocks + (row + rows) % row_blocks
                pairs.append((band * row_blocks + row, target))
        return lax.ppermute(value, axes, pairs)

    row_block = lax.axis_index(axes) % row_blocks
    flag = (row_block == row_blocks - 1).astype(jnp.int32).reshape(1)
    low, high = slice(0, half), slice(half, side)

    def piece(source, rows, columns, lanes):
        part = source[:, rows, columns, lanes]
        return part.reshape(3, half * half, part.shape[3])

    sizes = head_chunks(channels // HEAD_DIM)
    chunks = []
    start = 0
    for size in sizes:
        chunks.append(slice(start, start + size * HEAD_DIM))
        start += size * HEAD_DIM
    outgoing = []
    source = tokens
    for index, lanes in enumerate(chunks):
        sent = (
            piece(source, high, low, lanes),
            piece(source, low, high, lanes),
            piece(source, low, low, lanes),
        )
        if index == 0:
            source, sent = lax.optimization_barrier((source, sent))
        outgoing.append(sent)
    received = []
    for lanes, (east, south, corner) in zip(chunks, outgoing):
        received.append(
            (
                piece(source, high, high, lanes),
                shift(east, 0, -1),
                shift(south, -1, 0),
                shift(corner, -1, -1),
            )
        )
    results = []
    for quarters in received:
        own, east, south, corner = attend_quarters(flag, quarters)
        results.append((own, shift(east, 0, 1), shift(south, 1, 0), shift(corner, 1, 1)))
    return assemble(half, results).reshape(1, side, side, channels)


def solution(mesh):
    in_specs = (P(None, "win", "head", None, None),)
    out_specs = P("win", "head", None, None)
    win_count, head_count = mesh.shape["win"], mesh.shape["head"]

    def body(qkv):
        if qkv.shape[2] == qkv.shape[3]:
            return window_body(2 * head_count, win_count // 2, qkv)
        return general_body(qkv)

    return jax.shard_map(body, mesh=mesh, in_specs=in_specs, out_specs=out_specs, check_vma=False)
```
